256 devices in a mesh: ep: 16 (over z, core), fsdp: 4 (over x), tp: 4 (over y).
Axes of the slice: x: 4, y: 4, z: 8, core: 2. Of those that a mesh axis runs over, the one named last changes fastest.
Arguments:
- out_grad: bfloat16 [8192, 4096], P(('ep', 'fsdp')), may hold values from -1.5 to 1.5
- routes: int32 [8192, 2], P(('ep', 'fsdp')), may hold values from 0 to 15, all different within a row; in each aligned block of 128 rows (0 to 127, 128 to 255, ...) at most 32 rows name the same one
- chosen_logits: float32 [8192, 2], P(('ep', 'fsdp')), may hold values from -4 to 4
- routed_inputs: bfloat16 [16, 16, 4, 32, 4096], P('ep', None, 'fsdp'), may hold values from -6 to 6
- w_gate: bfloat16 [16, 4096, 1024], P('ep', 'fsdp', 'tp'), may hold values from -0.09375 to 0.09375
- w_up: bfloat16 [16, 4096, 1024], P('ep', 'fsdp', 'tp'), may hold values from -0.09375 to 0.09375
- w_down: bfloat16 [16, 1024, 4096], P('ep', 'tp', 'fsdp'), may hold values from -0.1875 to 0.1875
Outputs:
- input_grad: bfloat16 [8192, 4096], P(('ep', 'fsdp'))
- logit_grad: float32 [8192, 2], P(('ep', 'fsdp'))
- grad_gate: float32 [16, 4096, 1024], P('ep', 'fsdp', 'tp')
- grad_up: float32 [16, 4096, 1024], P('ep', 'fsdp', 'tp')
- grad_down: float32 [16, 1024, 4096], P('ep', 'tp', 'fsdp')
The draws below stay inside these ranges and needn't reach their ends.
Inputs may be any that keep to these rules, and one draw needn't show every extreme that they name: Each row of routes names 2 different experts. In each token group of 128 consecutive rows no expert is named by more than 32 rows, a bound that some block reaches.
All inputs are finite; a program needn't handle non-finite values.
Results may differ from the reference program's by a relative error of at most 0.015.
Values may be sent and summed in bfloat16 or wider, within the bound.
A program may use at most 128 MiB of HBM per device.

```python
import math
import jax
import jax.numpy as jnp
import numpy as np
from jax import lax

D = 4096
TOP = 2
FF = 1024
TOK_DEV = 128
EXPERTS = 16
SOURCES = 16
GROUPS = 4
CAPACITY = 32
TOKENS = 8192


def steps_of(key, extent, shards, least, top_value):
    factor_of = 1.0
    for axis_at, parts in shards:
        draws = jax.random.uniform(jax.random.fold_in(jax.random.fold_in(key, 6), axis_at), (parts,), jnp.float32, least / len(shards), top_value / len(shards))
        factor_of = factor_of * jnp.repeat(jnp.exp(draws), extent[axis_at] // parts).reshape((-1,) + (1,) * (len(extent) - 1 - axis_at))
    return factor_of


def shared_out(key, own, number, rows, amount, top, reach, skew):
    order = jax.random.permutation(key, amount)
    crowded, common = shares(amount, rows * top, reach, skew, True), shares(amount, rows * top, reach, skew, False)
    places = jnp.arange(amount)

    def named(sizes, rotation):
        used = int((sizes > 0).sum())
        fixed = max(1, used // 4)
        moved = fixed + (places - fixed + rotation * (used - fixed)) % max(1, amount - fixed)
        return jnp.zeros((amount,), jnp.int32).at[order[jnp.where(places < fixed, places, moved)]].set(jnp.asarray(sizes, jnp.int32))

    sizes = jnp.where(number % 4 == 0, named(crowded, number // 4), named(common, number - number // 4 - 1))
    mixed = jax.random.permutation(jax.random.fold_in(own, 3), amount)
    donor, receiver = mixed[0:amount // 2 * 2:2], mixed[1:amount // 2 * 2:2]
    room = jnp.minimum(sizes[donor] - 1, reach - sizes[receiver]) // 2
    room = jnp.where((donor == order[0]) | (receiver == order[0]) | (sizes[receiver] == 0), 0, jnp.maximum(room, 0))
    moved = jax.random.randint(jax.random.fold_in(own, 4), (amount // 2,), 0, 1 << 20) % (room + 1)
    sizes = sizes.at[donor].add(-moved).at[receiver].add(moved)
    labels = jnp.searchsorted(jnp.cumsum(sizes), jnp.arange(rows * top), side="right").astype(jnp.int32)
    grid = labels.reshape(top, rows).T
    grid = grid[jax.random.permutation(jax.random.fold_in(own, 1), rows)]
    rotation = jax.random.randint(jax.random.fold_in(own, 2), (rows, 1), 0, top)
    return jnp.take_along_axis(grid, (jnp.arange(top)[None, :] + rotation) % top, axis=1)


def shares(count, total, bound, slope, full):
    loads = [(1 << 20) // math.isqrt(standing ** slope) + 1 for standing in range(1, count + 1)]
    largest = bound if full else min(bound, max(-(-total // count), total * loads[0] // sum(loads)))
    least = 1 if total - largest >= count - 1 else 0
    holding, spare = [largest] + [least] * (count - 1), total - largest - least * (count - 1)
    while spare > 0:
        candidates = [i for i in range(1, count) if holding[i] < largest] or [i for i in range(1, count) if holding[i] < bound]
        mass, remaining = sum([loads[i] for i in candidates]), spare
        for i in candidates:
            more = min(bound - holding[i], max(1, remaining * loads[i] // mass), spare)
            holding[i] = holding[i] + more
            spare = spare - more
    return np.array(holding)


def scatter_about(own_key, dims, spread, reach, cuts=(), kind=jnp.bfloat16):
    drawn = jax.random.normal(own_key, dims, jnp.float32) * spread
    if len(cuts) > 0:
        drawn = steps_of(own_key, dims, cuts, -0.22, 0.18) * drawn
    return jnp.clip(drawn, min=-reach, max=reach).astype(kind)


def setup_inputs(seed: int = 0) -> dict:
    arg_keys = jax.random.split(jax.random.key(seed), 8)
    out_grad = scatter_about(arg_keys[0], (TOKENS, D), 0.25, 1.5, ((0, 64),))
    routes_keys = jax.random.split(jax.random.fold_in(arg_keys[1], 1), TOKENS // TOK_DEV)
    routes_turns = jax.random.permutation(jax.random.fold_in(arg_keys[1], 3), TOKENS // TOK_DEV)
    routes = jax.vmap(lambda own, number: shared_out(jax.random.fold_in(arg_keys[1], 2), own, number, TOK_DEV, EXPERTS, TOP, CAPACITY, 1))(routes_keys, routes_turns).reshape((TOKENS, TOP))
    chosen_logits = scatter_about(arg_keys[2], (TOKENS, TOP), 1.0, 4.0, ((0, 64),), jnp.float32)
    routed_inputs = scatter_about(arg_keys[3], (EXPERTS, SOURCES, GROUPS, CAPACITY, D), 1.0, 6.0, ((0, 16), (2, 4)))
    w_gate = scatter_about(arg_keys[4], (EXPERTS, D, FF), D ** -0.5, 0.09375, ((0, 16), (1, 4), (2, 4)))
    w_up = scatter_about(arg_keys[5], (EXPERTS, D, FF), D ** -0.5, 0.09375, ((0, 16), (1, 4), (2, 4)))
    w_down = scatter_about(arg_keys[6], (EXPERTS, FF, D), FF ** -0.5, 0.1875, ((0, 16), (1, 4), (2, 4)))
    return dict(out_grad=out_grad, routes=routes, chosen_logits=chosen_logits, routed_inputs=routed_inputs, w_gate=w_gate, w_up=w_up, w_down=w_down)


def group_slots(routes):
    flat_routes = routes.reshape(-1, TOK_DEV * TOP)
    onehot = (flat_routes[:, :, None] == jnp.arange(EXPERTS, dtype=jnp.int32)[None, None, :]).astype(jnp.int32)
    earlier = (jnp.cumsum(onehot, axis=1) - onehot).astype(jnp.int32)
    position = jnp.sum(earlier * onehot, axis=2).astype(jnp.int32)
    return (flat_routes * CAPACITY + position).astype(jnp.int32)


def take_rows(row_values, row_index):
    return jnp.take(row_values, row_index, axis=0)


def expert_pass(operands):
    inputs, scaled, gate_weight, up_weight, down_weight = operands
    gate_act = jnp.dot(inputs, gate_weight, preferred_element_type=jnp.float32)
    up_act = jnp.dot(inputs, up_weight, preferred_element_type=jnp.float32)
    sigmoid_gate = jax.nn.sigmoid(gate_act)
    silu_gate = gate_act * sigmoid_gate
    hidden = (silu_gate * up_act).astype(jnp.bfloat16)
    hidden_grad = jnp.dot(scaled, down_weight.T, preferred_element_type=jnp.float32)
    products = jnp.sum(hidden_grad * hidden.astype(jnp.float32), axis=1).astype(jnp.bfloat16)
    up_grad = (hidden_grad * silu_gate).astype(jnp.bfloat16)
    gate_grad = (hidden_grad * up_act * sigmoid_gate * (1.0 + gate_act * (1.0 - sigmoid_gate))).astype(jnp.bfloat16)
    grad_gate = jnp.dot(inputs.T, gate_grad, preferred_element_type=jnp.float32)
    grad_up = jnp.dot(inputs.T, up_grad, preferred_element_type=jnp.float32)
    grad_down = jnp.dot(hidden.T, scaled, preferred_element_type=jnp.float32)
    slot_grad = jnp.dot(gate_grad, gate_weight.T, preferred_element_type=jnp.float32)
    slot_grad = (slot_grad + jnp.dot(up_grad, up_weight.T, preferred_element_type=jnp.float32)).astype(jnp.bfloat16)
    return grad_gate, grad_up, grad_down, slot_grad, products


def reference(out_grad, routes, chosen_logits, routed_inputs, w_gate, w_up, w_down):
    groups = TOKENS // TOK_DEV
    pair_count = TOK_DEV * TOP
    gate_probs = jax.nn.softmax(chosen_logits, axis=-1)
    slot_index = group_slots(routes)
    weighted = (gate_probs[:, :, None] * out_grad.astype(jnp.float32)[:, None, :]).astype(jnp.bfloat16)
    weighted = weighted.reshape(groups, pair_count, D)
    weighted = jnp.concatenate([weighted, jnp.zeros((groups, 1, D), jnp.bfloat16)], axis=1)
    source = jnp.full((groups, EXPERTS * CAPACITY), pair_count, jnp.int32)
    group_rows = jnp.arange(groups, dtype=jnp.int32)[:, None]
    pair_ids = jnp.broadcast_to(jnp.arange(pair_count, dtype=jnp.int32)[None, :], (groups, pair_count))
    source = source.at[group_rows, slot_index].set(pair_ids)
    scaled = jax.vmap(take_rows)(weighted, source)
    scaled = scaled.reshape(groups, EXPERTS, CAPACITY, D).transpose(1, 0, 2, 3).reshape(EXPERTS, groups * CAPACITY, D)
    inputs = routed_inputs.reshape(EXPERTS, groups * CAPACITY, D)
    grad_gate, grad_up, grad_down, slot_grad, products = lax.map(expert_pass, (inputs, scaled, w_gate, w_up, w_down))
    slot_grad = slot_grad.reshape(EXPERTS, groups, CAPACITY, D).transpose(1, 0, 2, 3).reshape(groups, EXPERTS * CAPACITY, D)
    picked = jax.vmap(take_rows)(slot_grad, slot_index).astype(jnp.float32)
    input_grad = jnp.sum(picked.reshape(TOKENS, TOP, D), axis=1).astype(jnp.bfloat16)
    products = products.reshape(EXPERTS, groups, CAPACITY).transpose(1, 0, 2).reshape(groups, EXPERTS * CAPACITY)
    chosen = jnp.take_along_axis(products, slot_index, axis=1).astype(jnp.float32).reshape(TOKENS, TOP)
    logit_grad = chosen - gate_probs * jnp.sum(chosen, axis=1, keepdims=True)
    return (input_grad, logit_grad, grad_gate, grad_up, grad_down)
```

```python
import functools

import jax
import jax.numpy as jnp
from jax import lax
from jax.experimental import pallas as pl
from jax.experimental.pallas import tpu as pltpu
from jax.sharding import PartitionSpec as P

MESH = pl.DeviceIdType.MESH
F32, BF16, I32 = jnp.float32, jnp.bfloat16, jnp.int32

DZ = (0, 1, -1, 2, -2, 3, -3, 4)
NJ = 16
CAP = 32
TOK = 128
NCH = 4
ROWS = 128
SLOTS = 512
Q = 1024
FFL = 256


def dot_nn(a, b):
    return lax.dot_general(a, b, (((1,), (0,)), ((), ())), preferred_element_type=F32)


def dot_nt(a, b):
    return lax.dot_general(a, b, (((1,), (1,)), ((), ())), preferred_element_type=F32)


def kernel(
    routes, logits, og, x, wg, wu, wd,
    ig_o, lg_o, gg_o, gu_o, gd_o,
    xb, xt, wgb, wub, wdb, ogq, outb, sb,
    act_a, act_b, hg, hid, hidt, ggb, gub,
    qs, qt, q01, psb, m16, p16, c16,
    y1s, y1r, y2s, y2r, sown, ret, back,
    x1g, x1u, x1d, x1gr, x1ur, x1dr, x2g, x2u, x2d, x2gr, x2ur, x2dr, owng, ownu, ownd,
    fin, prt, prr, cs, cr,
    lx, lw, lo, so,
    xa_s, xa_r, xf_s, xf_r, x1_s, x1_rs, x2_s, x2_rs,
    ya_s, ya_r, yf_s, yf_r, y1_s, y1_rs, y2_s, y2_rs,
    za_s, za_r, zb_s, zb_r, zp_s, zp_r, fa_s, fa_r, ff_s, ff_r, c_s, c_r,
):
    ep = lax.axis_index("ep")
    f = lax.axis_index("fsdp")
    t = lax.axis_index("tp")
    z = ep // 2
    core = ep % 2

    def up(v):
        return (v + 1) % 4

    def down(v):
        return (v + 3) % 4

    xn = (up(f), down(f))
    yn = (up(t), down(t))

    def source_of(j):
        return ((z + DZ[j // 2] + 8) % 8) * 2 + (core + j % 2) % 2

    def expert_of(j):
        return ((z - DZ[j // 2] + 8) % 8) * 2 + (core + j % 2) % 2

    def remote(src, dst, ss, rs, **axis):
        return pltpu.make_async_remote_copy(
            src_ref=src, dst_ref=dst, send_sem=ss, recv_sem=rs, device_id=axis, device_id_type=MESH
        )

    tq = pl.multiple_of(t * Q, Q)
    l_og = pltpu.make_async_copy(og.at[:, pl.ds(tq, Q)], ogq, lo.at[0])
    l_w = [
        pltpu.make_async_copy(src, dst.at[f], lw.at[m])
        for m, (src, dst) in enumerate(((wg, wgb), (wu, wub), (wd, wdb)))
    ]
    l_w[0].start()
    l_w[1].start()
    l_og.start()
    l_x = [
        pltpu.make_async_copy(x.at[source_of(j)], xb.at[pl.ds(CAP * j, CAP), :], lx.at[j])
        for j in range(NJ)
    ]

    barrier = pltpu.get_barrier_semaphore()
    for k in (1, 3):
        pl.semaphore_signal(barrier, inc=1, device_id={"fsdp": (f + k) % 4}, device_id_type=MESH)
    for k in (1, 2, 3):
        pl.semaphore_signal(barrier, inc=1, device_id={"tp": (t + k) % 4}, device_id_type=MESH)
    for j in range(1, NJ):
        pl.semaphore_signal(barrier, inc=1, device_id={"ep": (ep + j) % 16}, device_id_type=MESH)
    l_w[2].start()
    for c in l_x:
        c.start()
    pl.semaphore_wait(barrier, 20)

    WB = (wgb, wub, wdb)
    HALF = (512, 512, 128)
    xa = [[remote(WB[m].at[f], WB[m].at[f], xa_s.at[m, d], xa_r.at[m, d], fsdp=xn[d]) for d in range(2)] for m in range(3)]

    def half_of(m, d, b):
        return WB[m].at[b, pl.ds(d * HALF[m], HALF[m]), :]

    fsrc = (down(f), up(f))
    xf = [
        [remote(half_of(m, d, fsrc[d]), half_of(m, d, fsrc[d]), xf_s.at[m, d], xf_r.at[m, d], fsdp=xn[d]) for d in range(2)]
        for m in range(3)
    ]

    def start(pair):
        for c in pair:
            c.start()

    for m in (0, 1):
        l_w[m].wait()
        start(xa[m])

    r0, r1 = routes[0:1, :], routes[1:2, :]
    g0, g1 = logits[0:1, :], logits[1:2, :]
    gm = jnp.maximum(g0, g1)
    e0, e1 = jnp.exp(g0 - gm), jnp.exp(g1 - gm)
    p0, p1 = e0 / (e0 + e1), e1 / (e0 + e1)
    jj = lax.broadcasted_iota(I32, (NJ, TOK), 0)
    ii = jj // 2
    dz = jnp.where(ii % 2 == 1, (ii + 1) // 2, -(ii // 2))
    ee = ((z - dz + 8) % 8) * 2 + (core + jj % 2) % 2
    h0, h1 = r0 == ee, r1 == ee
    m16[...] = jnp.where(h0, 1.0, 0.0) + jnp.where(h1, 2.0, 0.0)
    p16[...] = jnp.where(h0, p0, 0.0) + jnp.where(h1, p1, 0.0)
    taken = jnp.where(h0 | h1, 1.0, 0.0).astype(BF16)
    tri = jnp.where(
        lax.broadcasted_iota(I32, (TOK, TOK), 0) < lax.broadcasted_iota(I32, (TOK, TOK), 1), 1.0, 0.0
    ).astype(BF16)
    c16[...] = dot_nn(taken, tri)
    place = lax.broadcasted_iota(I32, (CAP, TOK), 0).astype(F32)
    for j in range(NJ):
        rows = pl.ds(CAP * j, CAP)
        code = m16[j : j + 1, :]
        here = c16[j : j + 1, :] == place
        one0 = jnp.where(here & (code == 1.0), 1.0, 0.0)
        one1 = jnp.where(here & (code == 2.0), 1.0, 0.0)
        q01[0, rows, :] = one0
        q01[1, rows, :] = one1
        one = one0 + one1
        qs[rows, :] = one.astype(BF16)
        psb[rows, :] = jnp.broadcast_to(jnp.sum(one * p16[j : j + 1, :], axis=1, keepdims=True), (CAP, TOK))
    l_og.wait()
    for c in range(NCH):
        rows = pl.ds(ROWS * c, ROWS)
        picked = dot_nn(qs[rows, :], ogq[...])
        outb[rows, :] = (picked * psb[rows, 0:1]).astype(BF16)

    za = [None] + [
        remote(
            outb.at[pl.ds(CAP * j, CAP), :], sb.at[t, pl.ds(CAP * j, CAP), :],
            za_s.at[j], za_r.at[j], ep=expert_of(j),
        )
        for j in range(1, NJ)
    ]
    for j in range(1, NJ):
        za[j].start()
    sb[t, 0:CAP, :] = outb[0:CAP, :]

    def add_block(dst, w, b, first):
        cols = pl.ds(pl.multiple_of(b * Q, Q), Q)

        @pl.loop(0, 2)
        def _(i):
            rows = pl.ds(pl.multiple_of(i * 256, 256), 256)
            part = dot_nn(xb[rows, cols], w[b])
            if first:
                dst[rows, :] = part
            else:
                dst[rows, :] += part

    for c in l_x:
        c.wait()
    add_block(act_a, wgb, f, True)

    ya = [
        [
            remote(sb.at[t, pl.ds(ROWS * c, ROWS), :], sb.at[t, pl.ds(ROWS * c, ROWS), :], ya_s.at[c, d], ya_r.at[c, d], tp=yn[d])
            for d in range(2)
        ]
        for c in range(NCH)
    ]
    tsrc = (down(t), up(t))

    def s_half(c, d):
        return sb.at[tsrc[d], pl.ds(ROWS * c + 64 * d, 64), :]

    yf = [[remote(s_half(c, d), s_half(c, d), yf_s.at[c, d], yf_r.at[c, d], tp=yn[d]) for d in range(2)] for c in range(NCH)]

    def rows_arrived(c):
        for j in range(max(1, 4 * c), 4 * c + 4):
            za[j].wait_recv()
        start(ya[c])

    def recv(pair):
        for c in pair:
            c.wait_recv()

    rows_arrived(0)
    add_block(act_b, wub, f, True)
    rows_arrived(1)
    recv(xa[0])
    start(xf[0])
    l_w[2].wait()
    start(xa[2])
    recv(ya[0])
    start(yf[0])
    add_block(act_a, wgb, up(f), False)
    add_block(act_a, wgb, down(f), False)
    rows_arrived(2)
    recv(ya[1])
    start(yf[1])

    def transpose_x(lo_, hi_):
        @pl.loop(lo_, hi_)
        def _(i):
            at = pl.ds(pl.multiple_of(i * 256, 256), 256)
            xt[at, :] = xb[:, at].T

    recv(xa[1])
    start(xf[1])
    add_block(act_b, wub, up(f), False)
    add_block(act_b, wub, down(f), False)
    rows_arrived(3)
    recv(ya[2])
    start(yf[2])
    transpose_x(0, 8)
    recv(xf[0])
    add_block(act_a, wgb, (f + 2) % 4, False)
    transpose_x(8, 16)
    recv(ya[3])
    start(yf[3])

    def add_hidden(b, first):
        @pl.loop(0, 2)
        def _(i):
            rows = pl.ds(pl.multiple_of(i * 256, 256), 256)
            part = dot_nt(sb[b, rows, :], wdb[b])
            if first:
                hg[rows, :] = part
            else:
                hg[rows, :] += part

    recv(xa[2])
    start(xf[2])
    for c in range(NCH):
        recv(yf[c])
    for k in (0, 1, 3):
        add_hidden((f + k) % 4, k == 0)
    qt[...] = qs[...].T
    recv(xf[1])
    add_block(act_b, wub, (f + 2) % 4, False)

    @pl.loop(0, 8)
    def _(i):
        rows = pl.ds(pl.multiple_of(i * 64, 64), 64)
        gate, upv = act_a[rows, :], act_b[rows, :]
        sig = jax.nn.sigmoid(gate)
        silu = gate * sig
        hid[rows, :] = (silu * upv).astype(BF16)
        act_a[rows, :] = silu
        act_b[rows, :] = upv * sig * (1.0 + gate * (1.0 - sig))

    hidt[...] = hid[...].T

    def x1_pair(m, s, r):
        h = HALF[m]
        return [
            remote(s.at[pl.ds(h * d, h), :], r.at[pl.ds(h * d, h), :], x1_s.at[m, d], x1_rs.at[m, d], fsdp=xn[d])
            for d in range(2)
        ]

    def x2_pair(m, s, r):
        return [remote(s.at[d], r.at[d], x2_s.at[m, d], x2_rs.at[m, d], fsdp=xn[d]) for d in range(2)]

    x1 = [x1_pair(0, x1g, x1gr), x1_pair(1, x1u, x1ur), x1_pair(2, x1d, x1dr)]
    x2 = [x2_pair(0, x2g, x2gr), x2_pair(1, x2u, x2ur), x2_pair(2, x2d, x2dr)]

    def down_grad(b, put):
        @pl.loop(0, 2)
        def _(i):
            cols = pl.ds(pl.multiple_of(i * 512, 512), 512)
            put(slice(None), cols, dot_nn(hidt[...], sb[b, :, cols]))

    def wide_grad(b, g, put):
        @pl.loop(0, 4)
        def _(i):
            rows = pl.ds(pl.multiple_of(i * 256, 256), 256)
            at = pl.ds(pl.multiple_of(b * Q + i * 256, 256), 256)
            put(rows, slice(None), dot_nn(xt[at, :], g[...]))

    def store_bf16(dst):
        def put(rows, cols, v):
            dst[rows, cols] = v.astype(BF16)

        return put

    def store_f32(dst):
        def put(rows, cols, v):
            dst[rows, cols] = v

        return put

    def add_half(m, dst, got):
        h = HALF[m]
        step = h // 2
        for d in range(2):

            @pl.loop(0, 2)
            def _(i):
                rows = pl.ds(pl.multiple_of(h * d + i * step, 64), step)
                dst[d, rows, :] = (dst[d, rows, :].astype(F32) + got[rows, :].astype(F32)).astype(BF16)

    down_grad((f + 2) % 4, store_bf16(x1d))
    start(x1[2])
    down_grad(up(f), store_bf16(x2d.at[0]))
    down_grad(down(f), store_bf16(x2d.at[1]))

    recv(xf[2])
    add_hidden((f + 2) % 4, False)

    for c in range(NCH):
        rows = pl.ds(ROWS * c, ROWS)
        h = hg[rows, :]
        gub[rows, :] = (h * act_a[rows, :]).astype(BF16)
        ggb[rows, :] = (h * act_b[rows, :]).astype(BF16)
        prod = jnp.sum(h * hid[rows, :].astype(F32), axis=1, keepdims=True)
        prt[c] = jnp.broadcast_to(prod, (ROWS, 128)).T[0:8, :]

    y1 = [
        [
            remote(y1s.at[c, pl.ds(64 * d, 64), :], y1r.at[c, pl.ds(64 * d, 64), :], y1_s.at[c, d], y1_rs.at[c, d], tp=yn[d])
            for d in range(2)
        ]
        for c in range(NCH)
    ]
    y2 = [[remote(y2s.at[c, d], y2r.at[c, d], y2_s.at[c, d], y2_rs.at[c, d], tp=yn[d]) for d in range(2)] for c in range(NCH)]

    def slot_block(c, b):
        rows = pl.ds(ROWS * c, ROWS)
        return dot_nt(ggb[rows, :], wgb[b]) + dot_nt(gub[rows, :], wub[b])

    def slot_first(c):
        y1s[c] = slot_block(c, (t + 2) % 4).astype(BF16)
        start(y1[c])

    def slot_rest(c):
        y2s[c, 0] = slot_block(c, up(t)).astype(BF16)
        y2s[c, 1] = slot_block(c, down(t)).astype(BF16)
        sown[pl.ds(ROWS * c, ROWS), :] = slot_block(c, t)

    def slot_second(c):
        recv(y1[c])
        for d in range(2):
            rows = pl.ds(64 * d, 64)
            y2s[c, d, rows, :] = (y2s[c, d, rows, :].astype(F32) + y1r[c, rows, :].astype(F32)).astype(BF16)
        start(y2[c])

    zb = [None] + [
        remote(ret.at[pl.ds(CAP * j, CAP), :], back.at[pl.ds(CAP * j, CAP), :], zb_s.at[j], zb_r.at[j], ep=source_of(j))
        for j in range(1, NJ)
    ]
    zp = [None] + [remote(prt.at[j // 4], prr.at[j], zp_s.at[j], zp_r.at[j], ep=source_of(j)) for j in range(1, NJ)]

    def slot_done(c):
        recv(y2[c])
        rows = pl.ds(ROWS * c, ROWS)
        total = sown[rows, :] + y2r[c, 0].astype(F32) + y2r[c, 1].astype(F32)
        ret[rows, :] = total.astype(BF16)
        for j in range(max(1, 4 * c), 4 * c + 4):
            zb[j].start()
        if c == 0:
            back[0:CAP, :] = ret[0:CAP, :]

    slot_first(3)
    wide_grad((f + 2) % 4, ggb, store_bf16(x1g))
    start(x1[0])
    slot_first(2)
    recv(x1[2])
    add_half(2, x2d, x1dr)
    start(x2[2])
    wide_grad((f + 2) % 4, gub, store_bf16(x1u))
    start(x1[1])
    slot_rest(3)
    slot_second(3)
    slot_first(1)
    slot_rest(2)
    slot_second(2)
    slot_first(0)
    for j in range(1, NJ):
        zp[j].start()
    prr[0] = prt[0]
    wide_grad(up(f), ggb, store_bf16(x2g.at[0]))
    wide_grad(down(f), ggb, store_bf16(x2g.at[1]))
    slot_rest(1)
    slot_second(1)
    recv(x1[0])
    add_half(0, x2g, x1gr)
    start(x2[0])
    slot_done(3)
    slot_rest(0)
    slot_second(0)
    wide_grad(up(f), gub, store_bf16(x2u.at[0]))
    wide_grad(down(f), gub, store_bf16(x2u.at[1]))
    recv(x1[1])
    add_half(1, x2u, x1ur)
    start(x2[1])
    slot_done(2)
    down_grad(f, store_f32(ownd))
    wide_grad(f, ggb, store_f32(owng))
    wide_grad(f, gub, store_f32(ownu))
    slot_done(1)

    outs = [
        pltpu.make_async_copy(owng, gg_o, so.at[0]),
        pltpu.make_async_copy(ownu, gu_o, so.at[1]),
        pltpu.make_async_copy(ownd, gd_o, so.at[2]),
    ]

    def finish(m, own, got):
        recv(x2[m])
        n = own.shape[0] // 4

        @pl.loop(0, 4)
        def _(i):
            rows = pl.ds(pl.multiple_of(i * n, 64), n)
            own[rows, :] = own[rows, :] + got[0, rows, :].astype(F32) + got[1, rows, :].astype(F32)

        outs[m].start()

    finish(2, ownd, x2dr)

    for j in range(1, NJ):
        zp[j].wait_recv()
    lane = lax.broadcasted_iota(I32, (8, 128), 1) // CAP
    ch = [jnp.zeros((8, TOK), F32), jnp.zeros((8, TOK), F32)]
    for c in range(NCH):
        row = jnp.zeros((8, 128), F32)
        for i in range(4):
            row = jnp.where(lane == i, prr[4 * c + i], row)
        for k in range(2):
            ch[k] = ch[k] + lax.dot_general(
                row, q01[k, pl.ds(ROWS * c, ROWS), :], (((1,), (0,)), ((), ())),
                precision=lax.Precision.HIGHEST, preferred_element_type=F32,
            )
    half8 = lax.broadcasted_iota(I32, (8, TOK), 0)
    cs[...] = jnp.where(half8 == 0, ch[0], ch[1])
    cc = [
        remote(cs, cr.at[t], c_s.at[k - 1], c_r.at[k - 1], tp=(t + k) % 4) for k in (1, 2, 3)
    ]
    start(cc)
    cr[t] = cs[...]

    slot_done(0)

    for j in range(1, NJ):
        zb[j].wait_recv()

    for i in range(2):
        cols = pl.ds(512 * i, 512)
        fin[t, :, cols] = dot_nn(qt[...], back[:, cols]).astype(BF16)
    fa = [remote(fin.at[t], fin.at[t], fa_s.at[d], fa_r.at[d], tp=yn[d]) for d in range(2)]

    def f_half(d):
        return fin.at[tsrc[d], pl.ds(64 * d, 64), :]

    ffw = [remote(f_half(d), f_half(d), ff_s.at[d], ff_r.at[d], tp=yn[d]) for d in range(2)]
    start(fa)
    recv(cc)
    total = ((cr[0] + cr[1]) + cr[2]) + cr[3]
    chosen = total.astype(BF16).astype(F32)
    both = chosen[0:1, :] + chosen[1:2, :]
    pp = jnp.where(half8 == 0, p0, p1)
    lg_o[...] = chosen - pp * both
    finish(0, owng, x2gr)
    o_own = pltpu.make_async_copy(fin.at[t], ig_o.at[:, pl.ds(tq, Q)], so.at[3])
    o_own.start()
    recv(fa)
    start(ffw)
    o_nb = []
    for d in range(2):
        at = pl.multiple_of(tsrc[d] * Q, Q)
        o_nb.append(pltpu.make_async_copy(fin.at[tsrc[d]], ig_o.at[:, pl.ds(at, Q)], so.at[4 + d]))
    start(o_nb)
    finish(1, ownu, x2ur)
    recv(ffw)
    opp = (t + 2) % 4
    o_op = pltpu.make_async_copy(fin.at[opp], ig_o.at[:, pl.ds(pl.multiple_of(opp * Q, Q), Q)], so.at[6])
    o_op.start()

    for group in (xa, xf, x1, x2, ya, yf, y1, y2):
        for pair in group:
            for c in pair:
                c.wait_send()
    for group in (za[1:], zb[1:], zp[1:], fa, ffw, cc):
        for c in group:
            c.wait_send()
    for c in outs + [o_own, o_op] + o_nb:
        c.wait()


def on_device(out_grad, routes, chosen_logits, routed_inputs, w_gate, w_up, w_down):
    hbm = pl.BlockSpec(memory_space=pl.ANY)
    vmem = pl.BlockSpec(memory_space=pltpu.VMEM)
    dma = pltpu.SemaphoreType.DMA

    def v(*shape, dtype=BF16):
        return pltpu.VMEM(shape, dtype)

    scratch = [
        v(SLOTS, 4 * Q), v(4 * Q, SLOTS), v(4, Q, FFL), v(4, Q, FFL), v(4, FFL, Q),
        v(TOK, Q), v(SLOTS, Q), v(4, SLOTS, Q),
        v(SLOTS, FFL, dtype=F32), v(SLOTS, FFL, dtype=F32), v(SLOTS, FFL, dtype=F32),
        v(SLOTS, FFL), v(FFL, SLOTS), v(SLOTS, FFL), v(SLOTS, FFL),
        v(SLOTS, TOK), v(TOK, SLOTS), v(2, SLOTS, TOK, dtype=F32), v(SLOTS, TOK, dtype=F32),
        v(NJ, TOK, dtype=F32), v(NJ, TOK, dtype=F32), v(NJ, TOK, dtype=F32),
        v(NCH, ROWS, Q), v(NCH, ROWS, Q), v(NCH, 2, ROWS, Q), v(NCH, 2, ROWS, Q),
        v(SLOTS, Q, dtype=F32), v(SLOTS, Q), v(SLOTS, Q),
        v(Q, FFL), v(Q, FFL), v(FFL, Q), v(Q, FFL), v(Q, FFL), v(FFL, Q),
        v(2, Q, FFL), v(2, Q, FFL), v(2, FFL, Q), v(2, Q, FFL), v(2, Q, FFL), v(2, FFL, Q),
        v(Q, FFL, dtype=F32), v(Q, FFL, dtype=F32), v(FFL, Q, dtype=F32),
        v(4, TOK, Q), v(NCH, 8, 128, dtype=F32), v(NJ, 8, 128, dtype=F32),
        v(8, 128, dtype=F32), v(4, 8, 128, dtype=F32),
        dma((NJ,)), dma((3,)), dma((1,)), dma((7,)),
        dma((3, 2)), dma((3, 2)), dma((3, 2)), dma((3, 2)), dma((3, 2)), dma((3, 2)), dma((3, 2)), dma((3, 2)),
        dma((4, 2)), dma((4, 2)), dma((4, 2)), dma((4, 2)), dma((4, 2)), dma((4, 2)), dma((4, 2)), dma((4, 2)),
        dma((NJ,)), dma((NJ,)), dma((NJ,)), dma((NJ,)), dma((NJ,)), dma((NJ,)),
        dma((2,)), dma((2,)), dma((2,)), dma((2,)), dma((3,)), dma((3,)),
    ]
    ig, lg, gg, gu, gd = pl.pallas_call(
        kernel,
        out_shape=(
            jax.ShapeDtypeStruct((TOK, 4 * Q), BF16),
            jax.ShapeDtypeStruct((8, 128), F32),
            jax.ShapeDtypeStruct((Q, FFL), F32),
            jax.ShapeDtypeStruct((Q, FFL), F32),
            jax.ShapeDtypeStruct((FFL, Q), F32),
        ),
        in_specs=[vmem, vmem, hbm, hbm, hbm, hbm, hbm],
        out_specs=(hbm, vmem, hbm, hbm, hbm),
        scratch_shapes=scratch,
        compiler_params=pltpu.CompilerParams(
            collective_id=0, has_side_effects=True, vmem_limit_bytes=60 * 1024 * 1024
        ),
    )(
        routes.T, chosen_logits.T, out_grad,
        routed_inputs.reshape(NJ, CAP, 4 * Q), w_gate[0], w_up[0], w_down[0],
    )
    return ig, lg[:2].T, gg[None], gu[None], gd[None]


def solution(mesh):
    return jax.shard_map(
        on_device,
        mesh=mesh,
        in_specs=(
            P(("ep", "fsdp"), None),
            P(("ep", "fsdp"), None),
            P(("ep", "fsdp"), None),
            P("ep", None, "fsdp", None, None),
            P("ep", "fsdp", "tp"),
            P("ep", "fsdp", "tp"),
            P("ep", "tp", "fsdp"),
        ),
        out_specs=(
            P(("ep", "fsdp"), None),
            P(("ep", "fsdp"), None),
            P("ep", "fsdp", "tp"),
            P("ep", "fsdp", "tp"),
            P("ep", "tp", "fsdp"),
        ),
        check_vma=False,
    )
```

```python
import functools

import jax
import jax.numpy as jnp
from jax import lax
from jax.experimental import pallas as pl
from jax.experimental.pallas import tpu as pltpu
from jax.sharding import PartitionSpec as P

MESH = pl.DeviceIdType.MESH
F32, BF16, I32 = jnp.float32, jnp.bfloat16, jnp.int32

DZ = (0, 1, -1, 2, -2, 3, -3, 4)
NJ = 16
CAP = 32
TOK = 128
NCH = 4
ROWS = 128
SLOTS = 512
Q = 1024
FFL = 256


def dot_nn(a, b):
    return lax.dot_general(a, b, (((1,), (0,)), ((), ())), preferred_element_type=F32)


def dot_nt(a, b):
    return lax.dot_general(a, b, (((1,), (1,)), ((), ())), preferred_element_type=F32)


def kernel(
    routes_in, logits_in, og, x, wg, wu, wd,
    ig_o, lg_o, gg_o, gu_o, gd_o,
    routes, logits, xb, xt, wgb, wub, wdb, ogq, outb, sb,
    act_a, act_b, hg, hid, hidt, ggb, gub,
    qs, qt, q01, psb, m16, p16, c16,
    y1s, y1r, y2s, y2r, sown, ret, back,
    x1g, x1u, x1d, x1gr, x1ur, x1dr, x2g, x2u, x2d, x2gr, x2ur, x2dr,
    prt, prr, cs, cr,
    lx, lw, lo, lv,
    xa_s, xa_r, xf_s, xf_r, x1_s, x1_rs, x2_s, x2_rs,
    ya_s, ya_r, yf_s, yf_r, y1_s, y1_rs, y2_s, y2_rs,
    za_s, za_r, zb_s, zb_r, zp_s, zp_r, fa_s, fa_r, ff_s, ff_r, c_s, c_r,
):
    ep = lax.axis_index("ep")
    f = lax.axis_index("fsdp")
    t = lax.axis_index("tp")
    z = ep // 2
    core = ep % 2

    def up(v):
        return (v + 1) % 4

    def down(v):
        return (v + 3) % 4

    xn = (up(f), down(f))
    yn = (up(t), down(t))

    def source_of(j):
        return ((z + DZ[j // 2] + 8) % 8) * 2 + (core + j % 2) % 2

    def expert_of(j):
        return ((z - DZ[j // 2] + 8) % 8) * 2 + (core + j % 2) % 2

    def remote(src, dst, ss, rs, **axis):
        return pltpu.make_async_remote_copy(
            src_ref=src, dst_ref=dst, send_sem=ss, recv_sem=rs, device_id=axis, device_id_type=MESH
        )

    tq = pl.multiple_of(t * Q, Q)
    l_og = pltpu.make_async_copy(og.at[:, pl.ds(tq, Q)], ogq, lo.at[0])
    l_r = [
        pltpu.make_async_copy(routes_in, routes, lo.at[1]),
        pltpu.make_async_copy(logits_in, logits, lo.at[2]),
    ]
    for c in l_r:
        c.start()
    l_og.start()
    l_w = [
        pltpu.make_async_copy(src, dst.at[f], lw.at[m])
        for m, (src, dst) in enumerate(((wg, wgb), (wu, wub), (wd, wdb)))
    ]
    l_x = [
        pltpu.make_async_copy(x.at[source_of(j)], xb.at[pl.ds(CAP * j, CAP), :], lx.at[j])
        for j in range(NJ)
    ]

    barrier = pltpu.get_barrier_semaphore()
    def tell(sem, **axis):
        pl.semaphore_signal(sem, inc=1, device_id=axis, device_id_type=MESH)

    zn = ((z + 1) % 8, (z + 7) % 8)
    for d in range(2):
        tell(barrier, fsdp=xn[d])
        tell(barrier, tp=yn[d])
        tell(barrier, ep=zn[d] * 2 + core)
        tell(barrier, ep=zn[d] * 2 + 1 - core)
    tell(barrier, ep=z * 2 + 1 - core)
    for c in l_w + l_x:
        c.start()
    pl.semaphore_wait(barrier, 9)

    def tell_level(k):
        for d in range(2):
            tell(lv.at[k, d], ep=zn[d] * 2 + core)

    def wait_level(k):
        for d in range(2):
            pl.semaphore_wait(lv.at[k, d], 1)

    tell_level(0)

    WIN = (wg, wu, wd)
    WB = (wgb, wub, wdb)
    HALF = (512, 512, 128)
    xa = [[remote(WIN[m], WB[m].at[f], xa_s.at[m, d], xa_r.at[m, d], fsdp=xn[d]) for d in range(2)] for m in range(3)]

    def half_of(m, d, b):
        return WB[m].at[b, pl.ds(d * HALF[m], HALF[m]), :]

    fsrc = (down(f), up(f))
    xf = [
        [remote(half_of(m, d, fsrc[d]), half_of(m, d, fsrc[d]), xf_s.at[m, d], xf_r.at[m, d], fsdp=xn[d]) for d in range(2)]
        for m in range(3)
    ]

    def start(pair):
        for c in pair:
            c.start()

    start(xa[0])
    start(xa[1])

    for c in l_r:
        c.wait()
    r0, r1 = routes[0:1, :], routes[1:2, :]
    g0, g1 = logits[0:1, :], logits[1:2, :]
    gm = jnp.maximum(g0, g1)
    e0, e1 = jnp.exp(g0 - gm), jnp.exp(g1 - gm)
    p0, p1 = e0 / (e0 + e1), e1 / (e0 + e1)
    jj = lax.broadcasted_iota(I32, (NJ, TOK), 0)
    ii = jj // 2
    dz = jnp.where(ii % 2 == 1, (ii + 1) // 2, -(ii // 2))
    ee = ((z - dz + 8) % 8) * 2 + (core + jj % 2) % 2
    h0, h1 = r0 == ee, r1 == ee
    m16[...] = jnp.where(h0, 1.0, 0.0) + jnp.where(h1, 2.0, 0.0)
    p16[...] = jnp.where(h0, p0, 0.0) + jnp.where(h1, p1, 0.0)
    taken = jnp.where(h0 | h1, 1.0, 0.0).astype(BF16)
    tri = jnp.where(
        lax.broadcasted_iota(I32, (TOK, TOK), 0) < lax.broadcasted_iota(I32, (TOK, TOK), 1), 1.0, 0.0
    ).astype(BF16)
    c16[...] = dot_nn(taken, tri)
    place = lax.broadcasted_iota(I32, (CAP, TOK), 0).astype(F32)
    for j in range(NJ):
        rows = pl.ds(CAP * j, CAP)
        code = m16[j : j + 1, :]
        here = c16[j : j + 1, :] == place
        one0 = jnp.where(here & (code == 1.0), 1.0, 0.0)
        one1 = jnp.where(here & (code == 2.0), 1.0, 0.0)
        q01[0, rows, :] = one0
        q01[1, rows, :] = one1
        one = one0 + one1
        qs[rows, :] = one.astype(BF16)
        psb[rows, :] = jnp.broadcast_to(jnp.sum(one * p16[j : j + 1, :], axis=1, keepdims=True), (CAP, TOK))
    l_og.wait()
    for c in range(NCH):
        rows = pl.ds(ROWS * c, ROWS)
        picked = dot_nn(qs[rows, :], ogq[...])
        outb[rows, :] = (picked * psb[rows, 0:1]).astype(BF16)

    za = [None] + [
        remote(
            outb.at[pl.ds(CAP * j, CAP), :], sb.at[t, pl.ds(CAP * j, CAP), :],
            za_s.at[j], za_r.at[j], ep=expert_of(j),
        )
        for j in range(1, NJ)
    ]
    start(za[1:6])
    wait_level(0)
    tell_level(1)
    start(za[6:10])
    wait_level(1)
    tell_level(2)
    start(za[10:14])
    wait_level(2)
    start(za[14:])
    sb[t, 0:CAP, :] = outb[0:CAP, :]
    for c in l_w:
        c.wait()

    def add_block(dst, w, b, first):
        cols = pl.ds(pl.multiple_of(b * Q, Q), Q)

        @pl.loop(0, 2)
        def _(i):
            rows = pl.ds(pl.multiple_of(i * 256, 256), 256)
            part = dot_nn(xb[rows, cols], w[b])
            if first:
                dst[rows, :] = part
            else:
                dst[rows, :] += part

    for c in l_x:
        c.wait()
    add_block(act_a, wgb, f, True)

    ya = [
        [
            remote(sb.at[t, pl.ds(ROWS * c, ROWS), :], sb.at[t, pl.ds(ROWS * c, ROWS), :], ya_s.at[c, d], ya_r.at[c, d], tp=yn[d])
            for d in range(2)
        ]
        for c in range(NCH)
    ]
    tsrc = (down(t), up(t))

    def s_half(c, d):
        return sb.at[tsrc[d], pl.ds(ROWS * c + 64 * d, 64), :]

    yf = [[remote(s_half(c, d), s_half(c, d), yf_s.at[c, d], yf_r.at[c, d], tp=yn[d]) for d in range(2)] for c in range(NCH)]

    def rows_arrived(c):
        for j in range(max(1, 4 * c), 4 * c + 4):
            za[j].wait_recv()
        start(ya[c])

    def recv(pair):
        for c in pair:
            c.wait_recv()

    rows_arrived(0)
    add_block(act_b, wub, f, True)
    rows_arrived(1)
    recv(xa[0])
    start(xf[0])
    start(xa[2])
    recv(ya[0])
    start(yf[0])
    add_block(act_a, wgb, up(f), False)
    add_block(act_a, wgb, down(f), False)
    rows_arrived(2)
    recv(ya[1])
    start(yf[1])

    def transpose_x(lo_, hi_):
        @pl.loop(lo_, hi_)
        def _(i):
            at = pl.ds(pl.multiple_of(i * 256, 256), 256)
            xt[at, :] = xb[:, at].T

    recv(xa[1])
    start(xf[1])
    add_block(act_b, wub, up(f), False)
    add_block(act_b, wub, down(f), False)
    rows_arrived(3)
    recv(ya[2])
    start(yf[2])
    transpose_x(0, 8)
    recv(xf[0])
    add_block(act_a, wgb, (f + 2) % 4, False)
    transpose_x(8, 16)
    recv(ya[3])
    start(yf[3])

    def add_hidden(b, first):
        @pl.loop(0, 2)
        def _(i):
            rows = pl.ds(pl.multiple_of(i * 256, 256), 256)
            part = dot_nt(sb[b, rows, :], wdb[b])
            if first:
                hg[rows, :] = part
            else:
                hg[rows, :] += part

    recv(xa[2])
    start(xf[2])
    for c in range(NCH):
        recv(yf[c])
    for k in (0, 1, 3):
        add_hidden((f + k) % 4, k == 0)
    qt[...] = qs[...].T
    recv(xf[1])
    add_block(act_b, wub, (f + 2) % 4, False)

    @pl.loop(0, 8)
    def _(i):
        rows = pl.ds(pl.multiple_of(i * 64, 64), 64)
        gate, upv = act_a[rows, :], act_b[rows, :]
        sig = jax.nn.sigmoid(gate)
        silu = gate * sig
        hid[rows, :] = (silu * upv).astype(BF16)
        act_a[rows, :] = silu
        act_b[rows, :] = upv * sig * (1.0 + gate * (1.0 - sig))

    hidt[...] = hid[...].T

    def x1_pair(m, s, r):
        h = HALF[m]
        return [
            remote(s.at[pl.ds(h * d, h), :], r.at[pl.ds(h * d, h), :], x1_s.at[m, d], x1_rs.at[m, d], fsdp=xn[d])
            for d in range(2)
        ]

    def x2_pair(m, s, r):
        return [remote(s.at[d], r.at[d], x2_s.at[m, d], x2_rs.at[m, d], fsdp=xn[d]) for d in range(2)]

    x1 = [x1_pair(0, x1g, x1gr), x1_pair(1, x1u, x1ur), x1_pair(2, x1d, x1dr)]
    x2 = [x2_pair(0, x2g, x2gr), x2_pair(1, x2u, x2ur), x2_pair(2, x2d, x2dr)]

    def down_grad(b, put):
        @pl.loop(0, 2)
        def _(i):
            cols = pl.ds(pl.multiple_of(i * 512, 512), 512)
            put(slice(None), cols, dot_nn(hidt[...], sb[b, :, cols]))

    def wide_grad(b, g, put):
        @pl.loop(0, 4)
        def _(i):
            rows = pl.ds(pl.multiple_of(i * 256, 256), 256)
            at = pl.ds(pl.multiple_of(b * Q + i * 256, 256), 256)
            put(rows, slice(None), dot_nn(xt[at, :], g[...]))

    def store_bf16(dst):
        def put(rows, cols, v):
            dst[rows, cols] = v.astype(BF16)

        return put

    def store_f32(dst):
        def put(rows, cols, v):
            dst[rows, cols] = v

        return put

    def add_half(m, dst, got):
        h = HALF[m]
        step = h // 2
        for d in range(2):

            @pl.loop(0, 2)
            def _(i):
                rows = pl.ds(pl.multiple_of(h * d + i * step, 64), step)
                dst[d, rows, :] = (dst[d, rows, :].astype(F32) + got[rows, :].astype(F32)).astype(BF16)

    down_grad((f + 2) % 4, store_bf16(x1d))
    start(x1[2])
    down_grad(up(f), store_bf16(x2d.at[0]))
    down_grad(down(f), store_bf16(x2d.at[1]))

    recv(xf[2])
    add_hidden((f + 2) % 4, False)

    for c in range(NCH):
        rows = pl.ds(ROWS * c, ROWS)
        h = hg[rows, :]
        gub[rows, :] = (h * act_a[rows, :]).astype(BF16)
        ggb[rows, :] = (h * act_b[rows, :]).astype(BF16)
        prod = jnp.sum(h * hid[rows, :].astype(F32), axis=1, keepdims=True)
        prt[c] = jnp.broadcast_to(prod, (ROWS, 128)).T[0:8, :]

    y1 = [
        [
            remote(y1s.at[c, pl.ds(64 * d, 64), :], y1r.at[c, pl.ds(64 * d, 64), :], y1_s.at[c, d], y1_rs.at[c, d], tp=yn[d])
            for d in range(2)
        ]
        for c in range(NCH)
    ]
    y2 = [[remote(y2s.at[c, d], y2r.at[c, d], y2_s.at[c, d], y2_rs.at[c, d], tp=yn[d]) for d in range(2)] for c in range(NCH)]

    def slot_block(c, b):
        rows = pl.ds(ROWS * c, ROWS)
        return dot_nt(ggb[rows, :], wgb[b]) + dot_nt(gub[rows, :], wub[b])

    def slot_first(c):
        y1s[c] = slot_block(c, (t + 2) % 4).astype(BF16)
        start(y1[c])

    def slot_rest(c):
        y2s[c, 0] = slot_block(c, up(t)).astype(BF16)
        y2s[c, 1] = slot_block(c, down(t)).astype(BF16)
        sown[pl.ds(ROWS * c, ROWS), :] = slot_block(c, t)

    def slot_second(c):
        recv(y1[c])
        for d in range(2):
            rows = pl.ds(64 * d, 64)
            y2s[c, d, rows, :] = (y2s[c, d, rows, :].astype(F32) + y1r[c, rows, :].astype(F32)).astype(BF16)
        start(y2[c])

    zb = [None] + [
        remote(ret.at[pl.ds(CAP * j, CAP), :], back.at[pl.ds(CAP * j, CAP), :], zb_s.at[j], zb_r.at[j], ep=source_of(j))
        for j in range(1, NJ)
    ]
    zp = [None] + [remote(prt.at[j // 4], prr.at[j], zp_s.at[j], zp_r.at[j], ep=source_of(j)) for j in range(1, NJ)]

    def slot_done(c):
        recv(y2[c])
        rows = pl.ds(ROWS * c, ROWS)
        total = sown[rows, :] + y2r[c, 0].astype(F32) + y2r[c, 1].astype(F32)
        ret[rows, :] = total.astype(BF16)
        for j in range(max(1, 4 * c), 4 * c + 4):
            zb[j].start()
        if c == 0:
            back[0:CAP, :] = ret[0:CAP, :]

    slot_first(3)
    slot_first(2)
    wide_grad((f + 2) % 4, ggb, store_bf16(x1g))
    start(x1[0])
    slot_rest(3)
    wide_grad((f + 2) % 4, gub, store_bf16(x1u))
    start(x1[1])
    slot_second(3)
    recv(x1[2])
    add_half(2, x2d, x1dr)
    start(x2[2])
    slot_first(1)
    slot_rest(2)
    slot_second(2)
    slot_first(0)
    for j in range(1, NJ):
        zp[j].start()
    prr[0] = prt[0]
    slot_rest(1)
    slot_rest(0)
    wide_grad(up(f), ggb, store_bf16(x2g.at[0]))
    wide_grad(down(f), ggb, store_bf16(x2g.at[1]))
    slot_done(3)
    slot_second(1)
    recv(x1[0])
    add_half(0, x2g, x1gr)
    start(x2[0])
    wide_grad(up(f), gub, store_bf16(x2u.at[0]))
    wide_grad(down(f), gub, store_bf16(x2u.at[1]))
    slot_done(2)
    slot_second(0)
    down_grad(f, store_f32(gd_o))
    wide_grad(f, ggb, store_f32(gg_o))
    slot_done(1)
    recv(x1[1])
    add_half(1, x2u, x1ur)
    start(x2[1])
    wide_grad(f, gub, store_f32(gu_o))

    def finish(m, own, got):
        recv(x2[m])
        n = own.shape[0] // 4

        @pl.loop(0, 4)
        def _(i):
            rows = pl.ds(pl.multiple_of(i * n, 64), n)
            own[rows, :] = own[rows, :] + got[0, rows, :].astype(F32) + got[1, rows, :].astype(F32)

    finish(2, gd_o, x2dr)

    for j in range(1, NJ):
        zp[j].wait_recv()
    lane = lax.broadcasted_iota(I32, (8, 128), 1) // CAP
    ch = [jnp.zeros((8, TOK), F32), jnp.zeros((8, TOK), F32)]
    for c in range(NCH):
        row = jnp.zeros((8, 128), F32)
        for i in range(4):
            row = jnp.where(lane == i, prr[4 * c + i], row)
        for k in range(2):
            ch[k] = ch[k] + lax.dot_general(
                row, q01[k, pl.ds(ROWS * c, ROWS), :], (((1,), (0,)), ((), ())),
                precision=lax.Precision.HIGHEST, preferred_element_type=F32,
            )
    half8 = lax.broadcasted_iota(I32, (8, TOK), 0)
    cs[...] = jnp.where(half8 == 0, ch[0], ch[1])
    cc = [
        remote(cs, cr.at[t], c_s.at[k - 1], c_r.at[k - 1], tp=(t + k) % 4) for k in (1, 2, 3)
    ]
    start(cc)
    cr[t] = cs[...]

    slot_done(0)

    for j in range(1, NJ):
        zb[j].wait_recv()

    def columns(b):
        return pl.ds(pl.multiple_of(b * Q, Q), Q)

    def part(b, h):
        return ig_o.at[pl.ds(64 * h, 64), columns(b)]

    fa = [[remote(part(t, h), part(t, h), fa_s.at[d, h], fa_r.at[d, h], tp=yn[d]) for h in range(2)] for d in range(2)]
    ffw = [remote(part(tsrc[d], d), part(tsrc[d], d), ff_s.at[d], ff_r.at[d], tp=yn[d]) for d in range(2)]
    for h in range(2):
        ig_o[pl.ds(64 * h, 64), columns(t)] = dot_nn(qt[pl.ds(64 * h, 64), :], back[...]).astype(BF16)
        fa[h][h].start()
    fa[0][1].start()
    fa[1][0].start()
    recv(cc)
    total = ((cr[0] + cr[1]) + cr[2]) + cr[3]
    chosen = total.astype(BF16).astype(F32)
    both = chosen[0:1, :] + chosen[1:2, :]
    pp = jnp.where(half8 == 0, p0, p1)
    lg_o[...] = (chosen - pp * both)[0:2, :]
    finish(0, gg_o, x2gr)
    for d in range(2):
        fa[d][d].wait_recv()
        ffw[d].start()
    finish(1, gu_o, x2ur)
    fa[0][1].wait_recv()
    fa[1][0].wait_recv()
    recv(ffw)

    for group in (xa, xf, x1, x2, ya, yf, y1, y2):
        for pair in group:
            for c in pair:
                c.wait_send()
    for group in (za[1:], zb[1:], zp[1:], fa[0], fa[1], ffw, cc):
        for c in group:
            c.wait_send()


def deliver(*refs):
    n = len(refs) // 2
    sems = refs[-1]
    copies = [pltpu.make_async_copy(refs[i], refs[n + i], sems.at[i]) for i in range(n)]
    for c in copies:
        c.start()
    for c in copies:
        c.wait()


def on_device(out_grad, routes, chosen_logits, routed_inputs, w_gate, w_up, w_down):
    hbm = pl.BlockSpec(memory_space=pl.ANY)
    vmem = pl.BlockSpec(memory_space=pltpu.VMEM)
    dma = pltpu.SemaphoreType.DMA

    def v(*shape, dtype=BF16):
        return pltpu.VMEM(shape, dtype)

    scratch = [
        v(2, TOK, dtype=I32), v(2, TOK, dtype=F32), v(SLOTS, 4 * Q), v(4 * Q, SLOTS), v(4, Q, FFL), v(4, Q, FFL), v(4, FFL, Q),
        v(TOK, Q), v(SLOTS, Q), v(4, SLOTS, Q),
        v(SLOTS, FFL, dtype=F32), v(SLOTS, FFL, dtype=F32), v(SLOTS, FFL, dtype=F32),
        v(SLOTS, FFL), v(FFL, SLOTS), v(SLOTS, FFL), v(SLOTS, FFL),
        v(SLOTS, TOK), v(TOK, SLOTS), v(2, SLOTS, TOK, dtype=F32), v(SLOTS, TOK, dtype=F32),
        v(NJ, TOK, dtype=F32), v(NJ, TOK, dtype=F32), v(NJ, TOK, dtype=F32),
        v(NCH, ROWS, Q), v(NCH, ROWS, Q), v(NCH, 2, ROWS, Q), v(NCH, 2, ROWS, Q),
        v(SLOTS, Q, dtype=F32), v(SLOTS, Q), v(SLOTS, Q),
        v(Q, FFL), v(Q, FFL), v(FFL, Q), v(Q, FFL), v(Q, FFL), v(FFL, Q),
        v(2, Q, FFL), v(2, Q, FFL), v(2, FFL, Q), v(2, Q, FFL), v(2, Q, FFL), v(2, FFL, Q),
        v(NCH, 8, 128, dtype=F32), v(NJ, 8, 128, dtype=F32),
        v(8, 128, dtype=F32), v(4, 8, 128, dtype=F32),
        dma((NJ,)), dma((3,)), dma((3,)), pltpu.SemaphoreType.REGULAR((3, 2)),
        dma((3, 2)), dma((3, 2)), dma((3, 2)), dma((3, 2)), dma((3, 2)), dma((3, 2)), dma((3, 2)), dma((3, 2)),
        dma((4, 2)), dma((4, 2)), dma((4, 2)), dma((4, 2)), dma((4, 2)), dma((4, 2)), dma((4, 2)), dma((4, 2)),
        dma((NJ,)), dma((NJ,)), dma((NJ,)), dma((NJ,)), dma((NJ,)), dma((NJ,)),
        dma((2, 2)), dma((2, 2)), dma((2,)), dma((2,)), dma((3,)), dma((3,)),
    ]
    shapes = (
        jax.ShapeDtypeStruct((TOK, 4 * Q), BF16),
        jax.ShapeDtypeStruct((2, TOK), F32),
        jax.ShapeDtypeStruct((Q, FFL), F32),
        jax.ShapeDtypeStruct((Q, FFL), F32),
        jax.ShapeDtypeStruct((FFL, Q), F32),
    )
    made = pl.pallas_call(
        kernel,
        out_shape=shapes,
        in_specs=[hbm] * 7,
        out_specs=(vmem,) * 5,
        scratch_shapes=scratch,
        compiler_params=pltpu.CompilerParams(
            collective_id=0, has_side_effects=True, vmem_limit_bytes=48 * 1024 * 1024
        ),
    )(*[
        pltpu.with_memory_space_constraint(a, pltpu.HBM)
        for a in (
            routes.T, chosen_logits.T, out_grad,
            routed_inputs.reshape(NJ, CAP, 4 * Q), w_gate[0], w_up[0], w_down[0],
        )
    ])
    ig, lg, gg, gu, gd = pl.pallas_call(
        deliver,
        out_shape=shapes,
        in_specs=[vmem] * 5,
        out_specs=(hbm,) * 5,
        scratch_shapes=[dma((5,))],
        compiler_params=pltpu.CompilerParams(vmem_limit_bytes=4 * 1024 * 1024),
    )(*made)
    return ig, lg.T, gg[None], gu[None], gd[None]


def solution(mesh):
    return jax.shard_map(
        on_device,
        mesh=mesh,
        in_specs=(
            P(("ep", "fsdp"), None),
            P(("ep", "fsdp"), None),
            P(("ep", "fsdp"), None),
            P("ep", None, "fsdp", None, None),
            P("ep", "fsdp", "tp"),
            P("ep", "fsdp", "tp"),
            P("ep", "tp", "fsdp"),
        ),
        out_specs=(
            P(("ep", "fsdp"), None),
            P(("ep", "fsdp"), None),
            P("ep", "fsdp", "tp"),
            P("ep", "fsdp", "tp"),
            P("ep", "tp", "fsdp"),
        ),
        check_vma=False,
    )
```

```python
import functools

import jax
import jax.numpy as jnp
from jax import lax
from jax.experimental import pallas as pl
from jax.experimental.pallas import tpu as pltpu
from jax.sharding import PartitionSpec as P

MESH = pl.DeviceIdType.MESH
F32, BF16, I32 = jnp.float32, jnp.bfloat16, jnp.int32

DZ = (0, 1, -1, 2, -2, 3, -3, 4)
NJ = 16
CAP = 32
TOK = 128
NCH = 4
NSUB = 8
ROWS = 128
SLOTS = 512
Q = 1024
FFL = 256


def dot_nn(a, b):
    return lax.dot_general(a, b, (((1,), (0,)), ((), ())), preferred_element_type=F32)


def dot_nt(a, b):
    return lax.dot_general(a, b, (((1,), (1,)), ((), ())), preferred_element_type=F32)


def kernel(
    routes_in, logits_in, og, x, wg, wu, wd,
    ig_o, lg_o, gg_o, gu_o, gd_o,
    routes, logits, xb, xt, wgb, wub, wdb, ogq, outb, sb,
    act_a, act_b, hg, hid, hidt, ggb, gub,
    qs, qt, q01, psb, m16, p16, c16,
    y1s, y1r, y2s, y2r, sown, ret, back,
    x1g, x1u, x1d, x1gr, x1ur, x1dr, x2g, x2u, x2d, x2gr, x2ur, x2dr,
    prt, prr, cs, cr,
    lx, lw, lo, lv, sent,
    xa_r, xf_r, x1_rs, x2_rs, ya_r, yf_r, y1_rs, y2_rs, za_r, zb_r, zp_r, fa_r, ff_r, c_r,
):
    ep = lax.axis_index("ep")
    f = lax.axis_index("fsdp")
    t = lax.axis_index("tp")
    z = ep // 2
    core = ep % 2

    def up(v):
        return (v + 1) % 4

    def down(v):
        return (v + 3) % 4

    xn = (up(f), down(f))
    yn = (up(t), down(t))

    def source_of(j):
        return ((z + DZ[j // 2] + 8) % 8) * 2 + (core + j % 2) % 2

    def expert_of(j):
        return ((z - DZ[j // 2] + 8) % 8) * 2 + (core + j % 2) % 2

    def remote(src, dst, ss, rs, **axis):
        return pltpu.make_async_remote_copy(
            src_ref=src, dst_ref=dst, send_sem=ss, recv_sem=rs, device_id=axis, device_id_type=MESH
        )

    def arrived(ref, sem):
        pltpu.make_async_copy(ref, ref, sem).wait()

    def kib(n):
        return xb.at[pl.ds(0, n // 8), :]

    tq = pl.multiple_of(t * Q, Q)
    l_og = pltpu.make_async_copy(og.at[:, pl.ds(tq, Q)], ogq, lo.at[0])
    l_r = [
        pltpu.make_async_copy(routes_in, routes, lo.at[1]),
        pltpu.make_async_copy(logits_in, logits, lo.at[2]),
    ]
    for c in l_r:
        c.start()
    l_og.start()
    l_w = [
        pltpu.make_async_copy(src, dst.at[f], lw.at[m])
        for m, (src, dst) in enumerate(((wg, wgb), (wu, wub), (wd, wdb)))
    ]
    l_x = [
        pltpu.make_async_copy(x.at[source_of(j)], xb.at[pl.ds(CAP * j, CAP), :], lx.at[0])
        for j in range(NJ)
    ]

    barrier = pltpu.get_barrier_semaphore()
    def tell(sem, **axis):
        pl.semaphore_signal(sem, inc=1, device_id=axis, device_id_type=MESH)

    zn = ((z + 1) % 8, (z + 7) % 8)
    for d in range(2):
        tell(barrier, fsdp=xn[d])
        tell(barrier, tp=yn[d])
        tell(barrier, ep=zn[d] * 2 + core)
        tell(barrier, ep=zn[d] * 2 + 1 - core)
    tell(barrier, ep=z * 2 + 1 - core)
    for c in l_w + l_x:
        c.start()
    pl.semaphore_wait(barrier, 9)

    def tell_level(k):
        for d in range(2):
            tell(lv.at[k, d], ep=zn[d] * 2 + core)

    def wait_level(k):
        for d in range(2):
            pl.semaphore_wait(lv.at[k, d], 1)

    tell_level(0)

    WIN = (wg, wu, wd)
    WB = (wgb, wub, wdb)
    HALF = (512, 512, 128)
    xa = [[remote(WIN[m], WB[m].at[f], sent.at[0], xa_r.at[m], fsdp=xn[d]) for d in range(2)] for m in range(3)]

    def half_of(m, d, b):
        return WB[m].at[b, pl.ds(d * HALF[m], HALF[m]), :]

    fsrc = (down(f), up(f))
    xf = [
        [remote(half_of(m, d, fsrc[d]), half_of(m, d, fsrc[d]), sent.at[1], xf_r.at[m], fsdp=xn[d]) for d in range(2)]
        for m in range(3)
    ]

    def start(pair):
        for c in pair:
            c.start()

    start(xa[0])
    start(xa[1])

    for c in l_r:
        c.wait()
    r0, r1 = routes[0:1, :], routes[1:2, :]
    g0, g1 = logits[0:1, :], logits[1:2, :]
    gm = jnp.maximum(g0, g1)
    e0, e1 = jnp.exp(g0 - gm), jnp.exp(g1 - gm)
    p0, p1 = e0 / (e0 + e1), e1 / (e0 + e1)
    jj = lax.broadcasted_iota(I32, (NJ, TOK), 0)
    ii = jj // 2
    dz = jnp.where(ii % 2 == 1, (ii + 1) // 2, -(ii // 2))
    ee = ((z - dz + 8) % 8) * 2 + (core + jj % 2) % 2
    h0, h1 = r0 == ee, r1 == ee
    m16[...] = jnp.where(h0, 1.0, 0.0) + jnp.where(h1, 2.0, 0.0)
    p16[...] = jnp.where(h0, p0, 0.0) + jnp.where(h1, p1, 0.0)
    taken = jnp.where(h0 | h1, 1.0, 0.0).astype(BF16)
    tri = jnp.where(
        lax.broadcasted_iota(I32, (TOK, TOK), 0) < lax.broadcasted_iota(I32, (TOK, TOK), 1), 1.0, 0.0
    ).astype(BF16)
    c16[...] = dot_nn(taken, tri)
    place = lax.broadcasted_iota(I32, (CAP, TOK), 0).astype(F32)
    for j in range(NJ):
        rows = pl.ds(CAP * j, CAP)
        code = m16[j : j + 1, :]
        here = c16[j : j + 1, :] == place
        one0 = jnp.where(here & (code == 1.0), 1.0, 0.0)
        one1 = jnp.where(here & (code == 2.0), 1.0, 0.0)
        q01[0, rows, :] = one0
        q01[1, rows, :] = one1
        one = one0 + one1
        qs[rows, :] = one.astype(BF16)
        psb[rows, :] = jnp.broadcast_to(jnp.sum(one * p16[j : j + 1, :], axis=1, keepdims=True), (CAP, TOK))
    l_og.wait()
    for c in range(NCH):
        rows = pl.ds(ROWS * c, ROWS)
        picked = dot_nn(qs[rows, :], ogq[...])
        outb[rows, :] = (picked * psb[rows, 0:1]).astype(BF16)

    za = [None] + [
        remote(
            outb.at[pl.ds(CAP * j, CAP), :], sb.at[t, pl.ds(CAP * j, CAP), :],
            sent.at[2], za_r.at[j // 4], ep=expert_of(j),
        )
        for j in range(1, NJ)
    ]
    start(za[1:6])
    wait_level(0)
    tell_level(1)
    start(za[6:10])
    wait_level(1)
    tell_level(2)
    start(za[10:14])
    wait_level(2)
    start(za[14:])
    sb[t, 0:CAP, :] = outb[0:CAP, :]
    for c in l_w:
        c.wait()

    def add_block(dst, w, b, first):
        cols = pl.ds(pl.multiple_of(b * Q, Q), Q)

        @pl.loop(0, 2)
        def _(i):
            rows = pl.ds(pl.multiple_of(i * 256, 256), 256)
            part = dot_nn(xb[rows, cols], w[b])
            if first:
                dst[rows, :] = part
            else:
                dst[rows, :] += part

    arrived(xb, lx.at[0])
    add_block(act_a, wgb, f, True)

    ya = [
        [
            remote(sb.at[t, pl.ds(ROWS * c, ROWS), :], sb.at[t, pl.ds(ROWS * c, ROWS), :], sent.at[3], ya_r.at[c], tp=yn[d])
            for d in range(2)
        ]
        for c in range(NCH)
    ]
    tsrc = (down(t), up(t))

    def s_half(c, d):
        return sb.at[tsrc[d], pl.ds(ROWS * c + 64 * d, 64), :]

    yf = [[remote(s_half(c, d), s_half(c, d), sent.at[4], yf_r.at[0], tp=yn[d]) for d in range(2)] for c in range(NCH)]

    def rows_arrived(c):
        first = CAP if c == 0 else 0
        arrived(sb.at[t, pl.ds(ROWS * c + first, ROWS - first), :], za_r.at[c])
        start(ya[c])

    rows_arrived(0)
    add_block(act_b, wub, f, True)
    rows_arrived(1)
    arrived(kib(1024), xa_r.at[0])
    start(xf[0])
    start(xa[2])
    arrived(kib(512), ya_r.at[0])
    start(yf[0])
    add_block(act_a, wgb, up(f), False)
    add_block(act_a, wgb, down(f), False)
    rows_arrived(2)
    arrived(kib(512), ya_r.at[1])
    start(yf[1])

    def transpose_x(lo_, hi_):
        @pl.loop(lo_, hi_)
        def _(i):
            at = pl.ds(pl.multiple_of(i * 256, 256), 256)
            xt[at, :] = xb[:, at].T

    arrived(kib(1024), xa_r.at[1])
    start(xf[1])
    add_block(act_b, wub, up(f), False)
    add_block(act_b, wub, down(f), False)
    rows_arrived(3)
    arrived(kib(512), ya_r.at[2])
    start(yf[2])
    transpose_x(0, 8)
    arrived(kib(512), xf_r.at[0])
    add_block(act_a, wgb, (f + 2) % 4, False)
    transpose_x(8, 16)
    arrived(kib(512), ya_r.at[3])
    start(yf[3])

    def add_hidden(b, first):
        @pl.loop(0, 2)
        def _(i):
            rows = pl.ds(pl.multiple_of(i * 256, 256), 256)
            part = dot_nt(sb[b, rows, :], wdb[b])
            if first:
                hg[rows, :] = part
            else:
                hg[rows, :] += part

    arrived(kib(1024), xa_r.at[2])
    start(xf[2])
    arrived(kib(1024), yf_r.at[0])
    for k in (0, 1, 3):
        add_hidden((f + k) % 4, k == 0)
    qt[...] = qs[...].T
    arrived(kib(512), xf_r.at[1])
    add_block(act_b, wub, (f + 2) % 4, False)

    @pl.loop(0, 8)
    def _(i):
        rows = pl.ds(pl.multiple_of(i * 64, 64), 64)
        gate, upv = act_a[rows, :], act_b[rows, :]
        sig = jax.nn.sigmoid(gate)
        silu = gate * sig
        hid[rows, :] = (silu * upv).astype(BF16)
        act_a[rows, :] = silu
        act_b[rows, :] = upv * sig * (1.0 + gate * (1.0 - sig))

    hidt[...] = hid[...].T

    def x1_pair(m, s, r):
        h = HALF[m]
        return [
            remote(s.at[pl.ds(h * d, h), :], r.at[pl.ds(h * d, h), :], sent.at[5], x1_rs.at[m], fsdp=xn[d])
            for d in range(2)
        ]

    def x2_pair(m, s, r):
        return [remote(s.at[d], r.at[d], sent.at[6], x2_rs.at[m], fsdp=xn[d]) for d in range(2)]

    x1 = [x1_pair(0, x1g, x1gr), x1_pair(1, x1u, x1ur), x1_pair(2, x1d, x1dr)]
    x2 = [x2_pair(0, x2g, x2gr), x2_pair(1, x2u, x2ur), x2_pair(2, x2d, x2dr)]

    def down_grad(b, put):
        @pl.loop(0, 2)
        def _(i):
            cols = pl.ds(pl.multiple_of(i * 512, 512), 512)
            put(slice(None), cols, dot_nn(hidt[...], sb[b, :, cols]))

    def wide_grad(b, g, put):
        @pl.loop(0, 4)
        def _(i):
            rows = pl.ds(pl.multiple_of(i * 256, 256), 256)
            at = pl.ds(pl.multiple_of(b * Q + i * 256, 256), 256)
            put(rows, slice(None), dot_nn(xt[at, :], g[...]))

    def store_bf16(dst):
        def put(rows, cols, v):
            dst[rows, cols] = v.astype(BF16)

        return put

    def store_f32(dst):
        def put(rows, cols, v):
            dst[rows, cols] = v

        return put

    def add_half(m, dst, got):
        h = HALF[m]
        step = h // 2
        for d in range(2):

            @pl.loop(0, 2)
            def _(i):
                rows = pl.ds(pl.multiple_of(h * d + i * step, 64), step)
                dst[d, rows, :] = (dst[d, rows, :].astype(F32) + got[rows, :].astype(F32)).astype(BF16)

    down_grad((f + 2) % 4, store_bf16(x1d))
    start(x1[2])
    down_grad(up(f), store_bf16(x2d.at[0]))
    down_grad(down(f), store_bf16(x2d.at[1]))

    arrived(kib(512), xf_r.at[2])
    add_hidden((f + 2) % 4, False)

    for c in range(NCH):
        rows = pl.ds(ROWS * c, ROWS)
        h = hg[rows, :]
        gub[rows, :] = (h * act_a[rows, :]).astype(BF16)
        ggb[rows, :] = (h * act_b[rows, :]).astype(BF16)
        prod = jnp.sum(h * hid[rows, :].astype(F32), axis=1, keepdims=True)
        prt[c] = jnp.broadcast_to(prod, (ROWS, 128)).T[0:8, :]

    y1 = [
        [
            remote(y1s.at[pl.ds(64 * i + 32 * d, 32), :], y1r.at[pl.ds(64 * i + 32 * d, 32), :], sent.at[7], y1_rs.at[i], tp=yn[d])
            for d in range(2)
        ]
        for i in range(NSUB)
    ]
    y2 = [
        [
            remote(y2s.at[d, pl.ds(64 * i, 64), :], y2r.at[d, pl.ds(64 * i, 64), :], sent.at[8], y2_rs.at[i], tp=yn[d])
            for d in range(2)
        ]
        for i in range(NSUB)
    ]

    def slot_block(c, b):
        rows = pl.ds(ROWS * c, ROWS)
        return dot_nt(ggb[rows, :], wgb[b]) + dot_nt(gub[rows, :], wub[b])

    def slot_first(c):
        y1s[pl.ds(ROWS * c, ROWS), :] = slot_block(c, (t + 2) % 4).astype(BF16)
        start(y1[2 * c + 1])
        start(y1[2 * c])

    def slot_rest(c):
        rows = pl.ds(ROWS * c, ROWS)
        y2s[0, rows, :] = slot_block(c, up(t)).astype(BF16)
        y2s[1, rows, :] = slot_block(c, down(t)).astype(BF16)
        sown[rows, :] = slot_block(c, t)

    def slot_second(i):
        arrived(kib(128), y1_rs.at[i])
        for d in range(2):
            rows = pl.ds(64 * i + 32 * d, 32)
            y2s[d, rows, :] = (y2s[d, rows, :].astype(F32) + y1r[rows, :].astype(F32)).astype(BF16)
        start(y2[i])

    zb = [None] + [
        remote(ret.at[pl.ds(CAP * j, CAP), :], back.at[pl.ds(CAP * j, CAP), :], sent.at[9], zb_r.at[0], ep=source_of(j))
        for j in range(1, NJ)
    ]
    zp = [None] + [remote(prt.at[j // 4], prr.at[j], sent.at[10], zp_r.at[0], ep=source_of(j)) for j in range(1, NJ)]

    def slot_done(i):
        arrived(kib(256), y2_rs.at[i])
        rows = pl.ds(64 * i, 64)
        total = sown[rows, :] + y2r[0, rows, :].astype(F32) + y2r[1, rows, :].astype(F32)
        ret[rows, :] = total.astype(BF16)
        for j in range(max(1, 2 * i), 2 * i + 2):
            zb[j].start()
        if i == 0:
            back[0:CAP, :] = ret[0:CAP, :]

    slot_first(3)
    slot_first(2)
    wide_grad((f + 2) % 4, ggb, store_bf16(x1g))
    start(x1[0])
    slot_rest(3)
    slot_second(7)
    wide_grad((f + 2) % 4, gub, store_bf16(x1u))
    start(x1[1])
    slot_second(6)
    arrived(kib(512), x1_rs.at[2])
    add_half(2, x2d, x1dr)
    start(x2[2])
    slot_first(1)
    slot_rest(2)
    slot_second(5)
    slot_second(4)
    slot_first(0)
    for j in range(1, NJ):
        zp[j].start()
    prr[0] = prt[0]
    slot_rest(1)
    slot_done(7)
    slot_rest(0)
    slot_done(6)
    wide_grad(up(f), ggb, store_bf16(x2g.at[0]))
    wide_grad(down(f), ggb, store_bf16(x2g.at[1]))
    slot_second(3)
    slot_second(2)
    arrived(kib(512), x1_rs.at[0])
    add_half(0, x2g, x1gr)
    start(x2[0])
    wide_grad(up(f), gub, store_bf16(x2u.at[0]))
    wide_grad(down(f), gub, store_bf16(x2u.at[1]))
    slot_done(5)
    slot_done(4)
    slot_second(1)
    slot_second(0)
    down_grad(f, store_f32(gd_o))
    slot_done(3)
    wide_grad(f, ggb, store_f32(gg_o))
    slot_done(2)
    arrived(kib(512), x1_rs.at[1])
    add_half(1, x2u, x1ur)
    start(x2[1])
    slot_done(1)
    wide_grad(f, gub, store_f32(gu_o))

    def finish(m, own, got):
        arrived(kib(1024), x2_rs.at[m])
        n = own.shape[0] // 4

        @pl.loop(0, 4)
        def _(i):
            rows = pl.ds(pl.multiple_of(i * n, 64), n)
            own[rows, :] = own[rows, :] + got[0, rows, :].astype(F32) + got[1, rows, :].astype(F32)

    finish(2, gd_o, x2dr)

    arrived(prr.at[pl.ds(1, NJ - 1)], zp_r.at[0])
    lane = lax.broadcasted_iota(I32, (8, 128), 1) // CAP
    ch = [jnp.zeros((8, TOK), F32), jnp.zeros((8, TOK), F32)]
    for c in range(NCH):
        row = jnp.zeros((8, 128), F32)
        for i in range(4):
            row = jnp.where(lane == i, prr[4 * c + i], row)
        for k in range(2):
            ch[k] = ch[k] + lax.dot_general(
                row, q01[k, pl.ds(ROWS * c, ROWS), :], (((1,), (0,)), ((), ())),
                precision=lax.Precision.HIGHEST, preferred_element_type=F32,
            )
    half8 = lax.broadcasted_iota(I32, (8, TOK), 0)
    cs[...] = jnp.where(half8 == 0, ch[0], ch[1])
    cc = [
        remote(cs, cr.at[t], sent.at[11], c_r.at[0], tp=(t + k) % 4) for k in (1, 2, 3)
    ]
    start(cc)
    cr[t] = cs[...]

    slot_done(0)

    arrived(back.at[pl.ds(CAP, SLOTS - CAP), :], zb_r.at[0])

    def columns(b):
        return pl.ds(pl.multiple_of(b * Q, Q), Q)

    def part(b, h):
        return ig_o.at[pl.ds(64 * h, 64), columns(b)]

    fa = [[remote(part(t, h), part(t, h), sent.at[12], fa_r.at[d, h], tp=yn[d]) for h in range(2)] for d in range(2)]
    ffw = [remote(part(tsrc[d], d), part(tsrc[d], d), sent.at[13], ff_r.at[0], tp=yn[d]) for d in range(2)]
    for h in range(2):
        ig_o[pl.ds(64 * h, 64), columns(t)] = dot_nn(qt[pl.ds(64 * h, 64), :], back[...]).astype(BF16)
        fa[h][h].start()
    fa[0][1].start()
    fa[1][0].start()
    arrived(cr.at[pl.ds(0, 3)], c_r.at[0])
    total = ((cr[0] + cr[1]) + cr[2]) + cr[3]
    chosen = total.astype(BF16).astype(F32)
    both = chosen[0:1, :] + chosen[1:2, :]
    pp = jnp.where(half8 == 0, p0, p1)
    lg_o[...] = (chosen - pp * both)[0:2, :]
    finish(0, gg_o, x2gr)
    for d in range(2):
        fa[d][d].wait_recv()
        ffw[d].start()
    finish(1, gu_o, x2ur)
    fa[0][1].wait_recv()
    fa[1][0].wait_recv()
    arrived(kib(256), ff_r.at[0])

    for i, n in ((0, 3072), (1, 1536), (3, 2048), (4, 1024), (5, 1536), (6, 3072), (7, 1024), (8, 2048), (12, 512), (13, 256)):
        arrived(kib(n), sent.at[i])
    arrived(outb.at[pl.ds(CAP, SLOTS - CAP), :], sent.at[2])
    arrived(ret.at[pl.ds(CAP, SLOTS - CAP), :], sent.at[9])
    arrived(prr.at[pl.ds(1, NJ - 1)], sent.at[10])
    arrived(cr.at[pl.ds(0, 3)], sent.at[11])


def deliver(*refs):
    n = len(refs) // 2
    sems = refs[-1]
    copies = [pltpu.make_async_copy(refs[i], refs[n + i], sems.at[i]) for i in range(n)]
    for c in copies:
        c.start()
    for c in copies:
        c.wait()


def on_device(out_grad, routes, chosen_logits, routed_inputs, w_gate, w_up, w_down):
    hbm = pl.BlockSpec(memory_space=pl.ANY)
    vmem = pl.BlockSpec(memory_space=pltpu.VMEM)
    dma = pltpu.SemaphoreType.DMA

    def v(*shape, dtype=BF16):
        return pltpu.VMEM(shape, dtype)

    scratch = [
        v(2, TOK, dtype=I32), v(2, TOK, dtype=F32), v(SLOTS, 4 * Q), v(4 * Q, SLOTS), v(4, Q, FFL), v(4, Q, FFL), v(4, FFL, Q),
        v(TOK, Q), v(SLOTS, Q), v(4, SLOTS, Q),
        v(SLOTS, FFL, dtype=F32), v(SLOTS, FFL, dtype=F32), v(SLOTS, FFL, dtype=F32),
        v(SLOTS, FFL), v(FFL, SLOTS), v(SLOTS, FFL), v(SLOTS, FFL),
        v(SLOTS, TOK), v(TOK, SLOTS), v(2, SLOTS, TOK, dtype=F32), v(SLOTS, TOK, dtype=F32),
        v(NJ, TOK, dtype=F32), v(NJ, TOK, dtype=F32), v(NJ, TOK, dtype=F32),
        v(SLOTS, Q), v(SLOTS, Q), v(2, SLOTS, Q), v(2, SLOTS, Q),
        v(SLOTS, Q, dtype=F32), v(SLOTS, Q), v(SLOTS, Q),
        v(Q, FFL), v(Q, FFL), v(FFL, Q), v(Q, FFL), v(Q, FFL), v(FFL, Q),
        v(2, Q, FFL), v(2, Q, FFL), v(2, FFL, Q), v(2, Q, FFL), v(2, Q, FFL), v(2, FFL, Q),
        v(NCH, 8, 128, dtype=F32), v(NJ, 8, 128, dtype=F32),
        v(8, 128, dtype=F32), v(4, 8, 128, dtype=F32),
        dma((1,)), dma((3,)), dma((3,)), pltpu.SemaphoreType.REGULAR((3, 2)), dma((14,)),
        dma((3,)), dma((3,)), dma((3,)), dma((3,)), dma((NCH,)), dma((1,)), dma((NSUB,)), dma((NSUB,)),
        dma((NCH,)), dma((1,)), dma((1,)), dma((2, 2)), dma((1,)), dma((1,)),
    ]
    shapes = (
        jax.ShapeDtypeStruct((TOK, 4 * Q), BF16),
        jax.ShapeDtypeStruct((2, TOK), F32),
        jax.ShapeDtypeStruct((Q, FFL), F32),
        jax.ShapeDtypeStruct((Q, FFL), F32),
        jax.ShapeDtypeStruct((FFL, Q), F32),
    )
    made = pl.pallas_call(
        kernel,
        out_shape=shapes,
        in_specs=[hbm] * 7,
        out_specs=(vmem,) * 5,
        scratch_shapes=scratch,
        compiler_params=pltpu.CompilerParams(
            collective_id=0, has_side_effects=True, vmem_limit_bytes=48 * 1024 * 1024
        ),
    )(*[
        pltpu.with_memory_space_constraint(a, pltpu.HBM)
        for a in (
            routes.T, chosen_logits.T, out_grad,
            routed_inputs.reshape(NJ, CAP, 4 * Q), w_gate[0], w_up[0], w_down[0],
        )
    ])
    ig, lg, gg, gu, gd = pl.pallas_call(
        deliver,
        out_shape=shapes,
        in_specs=[vmem] * 5,
        out_specs=(hbm,) * 5,
        scratch_shapes=[dma((5,))],
        compiler_params=pltpu.CompilerParams(vmem_limit_bytes=4 * 1024 * 1024),
    )(*made)
    return ig, lg.T, gg[None], gu[None], gd[None]


def solution(mesh):
    return jax.shard_map(
        on_device,
        mesh=mesh,
        in_specs=(
            P(("ep", "fsdp"), None),
            P(("ep", "fsdp"), None),
            P(("ep", "fsdp"), None),
            P("ep", None, "fsdp", None, None),
            P("ep", "fsdp", "tp"),
            P("ep", "fsdp", "tp"),
            P("ep", "tp", "fsdp"),
        ),
        out_specs=(
            P(("ep", "fsdp"), None),
            P(("ep", "fsdp"), None),
            P("ep", "fsdp", "tp"),
            P("ep", "fsdp", "tp"),
            P("ep", "tp", "fsdp"),
        ),
        check_vma=False,
    )
```
